32 devices in a mesh: dp: 8 (over y, x, core), tensor: 4 (over z).
Axes of the slice: x: 2, y: 2, z: 4, core: 2. Of those that a mesh axis runs over, the one named last changes fastest.
Arguments:
- rollout: bfloat16 [2048, 6144], P('dp', 'tensor'), may hold values from -100 to 100
- lengths: int32 [8, 32], replicated, may hold values from 1 to 8, as said below
- packing: int32 [256], replicated, may hold values from 0 to 255, as said below
- norm_gain: float32 [6144], replicated, may hold values from 0.5 to 4
- query_weight: bfloat16 [6144, 1024], P(None, 'tensor'), may hold values from -0.078125 to 0.078125
- keyval_weight: bfloat16 [6144, 256], P(None, 'tensor'), may hold values from -0.078125 to 0.078125
- out_weight: bfloat16 [1024, 6144], P('tensor'), may hold values from -0.1875 to 0.1875
Outputs:
- layer_out: bfloat16 [2048, 6144], P('dp', 'tensor')
The draws below stay inside these ranges and needn't reach their ends.
Inputs may be any that keep to these rules, and one draw needn't show every extreme that they name: lengths[s, k] is the number of tokens of response k of source s; some response has 8 tokens in every draw. `packing`: a permutation of 0 .. 255; response r comes from source r // 32; every owner receives exactly 32 responses, exactly 4 of them from each source.
All inputs are finite; a program needn't handle non-finite values.
Results may differ from the reference program's by a relative error of at most 0.015.
Values may be sent and summed in bfloat16 or wider, within the bound.
A program may use at most 64 MiB of HBM per device.

```python
import math
import jax
import jax.numpy as jnp
from jax import lax

D = 6144
HD = 128
HQ_DEV = 2
GROUP = 8
MAXLEN = 8
RPS = 32
HEADS = 8
KV_HEADS = 1
L = 256
N_DP = 8
N_TENSOR = 4


def draw_lengths(key, part):
    drawn = jax.random.randint(jax.random.fold_in(key, 11), (N_DP * RPS,), 1, MAXLEN + 1)
    longest = jax.random.randint(jax.random.fold_in(key, 12), (), 0, N_DP * RPS)
    flattened = jnp.where(jnp.arange(N_DP * RPS) == longest, MAXLEN, drawn)
    return flattened.reshape(N_DP, RPS).astype(jnp.int32)


def draw_packing(key, part):
    response_count = N_DP * RPS
    owner_order = jax.random.permutation(jax.random.fold_in(key, 21), N_DP)
    source = jnp.arange(response_count) // RPS
    within = jnp.arange(response_count) % RPS
    target = owner_order[(source + within) % N_DP]
    tiebreak = jax.random.permutation(jax.random.fold_in(key, 22), response_count)
    sort_key = target * response_count + tiebreak
    return jnp.argsort(sort_key).astype(jnp.int32)


def draw_rollout(key, part):
    noise = jax.random.normal(jax.random.fold_in(key, 31), (N_DP * L, D), jnp.float32)
    return jnp.clip(noise, -100.0, 100.0).astype(jnp.bfloat16)


def draw_norm_gain(key, part):
    drawn = 1.0 + 0.1 * jax.random.normal(jax.random.fold_in(key, 42), (D,), jnp.float32)
    return jnp.clip(drawn, 0.5, 4.0).astype(jnp.float32)


def shard_levels(rng, shape, cuts, least, high):
    gain, own = 1.0, jax.random.fold_in(rng, 6)
    for axis_at, blocks in cuts:
        steps = jnp.exp(jax.random.uniform(jax.random.fold_in(own, axis_at), (blocks,), jnp.float32, least / len(cuts), high / len(cuts)))
        gain = gain * jnp.repeat(steps, shape[axis_at] // blocks).reshape([-1 if axis == axis_at else 1 for axis in range(len(shape))])
    return gain


def centred(own_key, shape, scale, most, shards=(), kind=jnp.bfloat16):
    gain = shard_levels(own_key, shape, shards, -0.22, 0.18) if shards else 1.0
    array = jax.random.normal(own_key, shape, jnp.float32) * scale * gain
    return jnp.minimum(jnp.maximum(array, -most), most).astype(kind)


def setup_inputs(seed: int = 0) -> dict:
    key_of = jax.random.split(jax.random.key(seed), 8)
    rollout = draw_rollout(jax.random.fold_in(key_of[7], 71), 0)
    lengths = draw_lengths(jax.random.fold_in(key_of[7], 71), 0)
    packing = draw_packing(jax.random.fold_in(key_of[7], 71), 0)
    norm_gain = draw_norm_gain(jax.random.fold_in(key_of[7], 71), 0)
    query_weight = centred(key_of[4], (D, HEADS * HD), D ** -0.5, 0.078125, ((1, 4),))
    keyval_weight = centred(key_of[5], (D, 2 * KV_HEADS * HD), D ** -0.5, 0.078125, ((1, 4),))
    out_weight = centred(key_of[6], (HEADS * HD, D), (HEADS * HD) ** -0.5, 0.1875, ((0, 4),))
    return {"rollout": rollout, "lengths": lengths, "packing": packing, "norm_gain": norm_gain, "query_weight": query_weight, "keyval_weight": keyval_weight, "out_weight": out_weight}


epsilon = 1e-05
rope_base = 500000.0

def owner_map(lengths, packing, owner_id, pack_len):
    per_source = lengths.shape[1]
    chosen = lax.dynamic_slice_in_dim(packing, owner_id * per_source, per_source)
    ordered = jnp.take(lengths.reshape(-1), chosen)
    doc_start = jnp.cumsum(ordered) - ordered
    places = jnp.arange(pack_len, dtype=jnp.int32)
    inside = (places[:, None] >= doc_start[None, :]) & (places[:, None] < (doc_start + ordered)[None, :])
    is_valid = jnp.any(inside, axis=1)
    slot_of = lax.optimization_barrier(jnp.sum(jnp.where(inside, jnp.arange(per_source, dtype=jnp.int32)[None, :], 0), axis=1)).astype(jnp.int32)
    response = jnp.take(chosen, slot_of)
    position = jnp.where(is_valid, places - jnp.take(doc_start, slot_of), 0).astype(jnp.int32)
    doc_id = jnp.where(is_valid, slot_of, per_source).astype(jnp.int32)
    return (response, position, doc_id, is_valid)

def rotate(values, position, head_dim):
    half_dim = head_dim // 2
    frequency = rope_base ** (-jnp.arange(half_dim, dtype=jnp.float32) * 2.0 / head_dim)
    angles = position.astype(jnp.float32)[:, None] * frequency[None, :]
    cosine = jnp.concatenate([jnp.cos(angles), jnp.cos(angles)], axis=1)[:, None, :]
    sine_table = jnp.concatenate([jnp.sin(angles), jnp.sin(angles)], axis=1)[:, None, :]
    turned = jnp.concatenate([-values[..., half_dim:], values[..., :half_dim]], axis=-1)
    return values * cosine + turned * sine_table

def reference(rollout, lengths, packing, norm_gain, query_weight, keyval_weight, out_weight):
    per_source = lengths.shape[1]
    source_start = (jnp.cumsum(lengths, axis=1) - lengths).reshape(-1).astype(jnp.int32)
    kv_count = keyval_weight.shape[1] // (2 * HD)
    head_count = query_weight.shape[1] // HD

    def one_owner(owner_id):
        response, position, doc_id, is_valid = owner_map(lengths, packing, owner_id, L)
        global_row = response // per_source * L + jnp.take(source_start, response) + position
        packed = jnp.where(is_valid[:, None], jnp.take(rollout, global_row.astype(jnp.int32), axis=0), jnp.zeros((), jnp.bfloat16))
        widened = packed.astype(jnp.float32)
        inverse = lax.rsqrt(lax.optimization_barrier(jnp.mean(widened * widened, axis=1)) + epsilon)
        scaled = (widened * norm_gain[None, :]).astype(jnp.bfloat16)
        queries = jnp.dot(scaled, query_weight, preferred_element_type=jnp.float32) * inverse[:, None]
        keyval = (jnp.dot(scaled, keyval_weight, preferred_element_type=jnp.float32) * inverse[:, None]).astype(jnp.bfloat16)
        q_rot = rotate(queries.reshape(L, head_count, HD), position, HD).astype(jnp.bfloat16)
        k_rot = rotate(keyval[:, :kv_count * HD].astype(jnp.float32).reshape(L, kv_count, HD), position, HD).astype(jnp.bfloat16)
        value_heads = keyval[:, kv_count * HD:].reshape(L, kv_count, HD)
        shared_head = jnp.arange(head_count, dtype=jnp.int32) // GROUP
        key_full = k_rot[:, shared_head]
        value_full = value_heads[:, shared_head]
        scores = jnp.einsum('qhd,khd->hqk', q_rot.astype(jnp.float32), key_full.astype(jnp.float32)) / math.sqrt(HD)
        places = jnp.arange(L, dtype=jnp.int32)
        allowed = (doc_id[:, None] == doc_id[None, :]) & (places[None, :] <= places[:, None])
        masked = jnp.where(allowed[None], scores, -jnp.inf)
        row_max = lax.optimization_barrier(jnp.max(masked, axis=2, keepdims=True))
        exponent = jnp.exp(masked - row_max)
        weights = (exponent / lax.optimization_barrier(jnp.sum(exponent, axis=2, keepdims=True))).astype(jnp.bfloat16)
        context = jnp.einsum('hqk,khd->qhd', weights.astype(jnp.float32), value_full.astype(jnp.float32))
        context = context.astype(jnp.bfloat16).reshape(L, head_count * HD)
        groups = context.reshape(L, N_TENSOR, HQ_DEV * HD).transpose(1, 0, 2)
        out_groups = out_weight.reshape(N_TENSOR, HQ_DEV * HD, D)

        def add_group(summed, operands):
            portion = jnp.dot(operands[0], operands[1], preferred_element_type=jnp.float32).astype(jnp.bfloat16)
            portion = lax.optimization_barrier(portion)
            return (summed + portion.astype(jnp.float32), None)
        summed, unused = lax.scan(add_group, jnp.zeros((L, D), jnp.float32), (groups, out_groups))
        return jnp.where(is_valid[:, None], summed + widened, 0.0).astype(jnp.bfloat16)
    outputs = lax.map(one_owner, jnp.arange(N_DP, dtype=jnp.int32))
    return outputs.reshape(N_DP * L, D)
```

```python
import functools
import math

import numpy as np
import jax
import jax.numpy as jnp
from jax import lax
from jax.experimental import pallas as pl
from jax.experimental.pallas import tpu as pltpu
from jax.sharding import PartitionSpec as P

D = 6144
HD = 128
HQ_DEV = 2
GROUP = 8


epsilon = 1e-05
rope_base = 500000.0


def owner_map(lengths, packing, owner_id, pack_len):
    per_source = lengths.shape[1]
    chosen = lax.dynamic_slice_in_dim(packing, owner_id * per_source, per_source)
    ordered = jnp.take(lengths.reshape(-1), chosen)
    doc_start = jnp.cumsum(ordered) - ordered
    places = jnp.arange(pack_len, dtype=jnp.int32)
    inside = (places[:, None] >= doc_start[None, :]) & (
        places[:, None] < (doc_start + ordered)[None, :]
    )
    is_valid = jnp.any(inside, axis=1)
    slot_of = jnp.sum(
        jnp.where(inside, jnp.arange(per_source, dtype=jnp.int32)[None, :], 0), axis=1
    )
    response = jnp.take(chosen, slot_of)
    position = jnp.where(is_valid, places - jnp.take(doc_start, slot_of), 0)
    doc_id = jnp.where(is_valid, slot_of, per_source)
    return (response, position, doc_id, is_valid)


def rotate(values, position, head_dim):
    half_dim = head_dim // 2
    frequency = rope_base ** (-jnp.arange(half_dim, dtype=jnp.float32) * 2.0 / head_dim)
    angles = position.astype(jnp.float32)[:, None] * frequency[None, :]
    cosine = jnp.concatenate([jnp.cos(angles), jnp.cos(angles)], axis=1)[:, None, :]
    sine_table = jnp.concatenate([jnp.sin(angles), jnp.sin(angles)], axis=1)[:, None, :]
    turned = jnp.concatenate([-values[..., half_dim:], values[..., :half_dim]], axis=-1)
    return values * cosine + turned * sine_table


def plain_body(rollout, lengths, packing, norm_gain, query_weight, keyval_weight, out_weight):
    owner_id = lax.axis_index("dp")
    tensor_index = lax.axis_index("tensor")
    tensor_count = lax.axis_size("tensor")
    pack_len = rollout.shape[0]
    per_source = lengths.shape[1]
    response, position, doc_id, is_valid = owner_map(lengths, packing, owner_id, pack_len)
    source_start = jnp.cumsum(lengths, axis=1) - lengths
    global_row = (
        response // per_source * pack_len + jnp.take(source_start.reshape(-1), response) + position
    )
    portion = lax.all_gather(rollout, "dp", axis=0, tiled=True)
    within = is_valid & (global_row >= 0) & (global_row < portion.shape[0])
    picked = jnp.take(portion, jnp.clip(global_row, 0, portion.shape[0] - 1), axis=0)
    packed = jnp.where(within[:, None], picked, jnp.zeros_like(rollout))
    widened = lax.all_gather(packed, "tensor", axis=1, tiled=True).astype(jnp.float32)
    scaled = (widened * norm_gain[None, :]).astype(jnp.bfloat16)
    query_acc = jnp.dot(scaled, query_weight, preferred_element_type=jnp.float32)
    keyval_acc = jnp.dot(scaled, keyval_weight, preferred_element_type=jnp.float32)
    squares = jnp.sum(widened * widened, axis=1)
    query_acc, keyval_acc, squares = (query_acc, keyval_acc, squares)
    inverse = lax.rsqrt(squares / D + epsilon)
    queries = query_acc * inverse[:, None]
    keyval_share = (keyval_acc * inverse[:, None]).astype(jnp.bfloat16)
    keyval_all = lax.all_gather(keyval_share, "tensor", axis=1, tiled=True)
    kv_count = keyval_weight.shape[1] * tensor_count // (2 * HD)
    shared_head = tensor_index * HQ_DEV // GROUP
    keys = lax.dynamic_slice_in_dim(keyval_all, shared_head * HD, HD, 1)
    values = lax.dynamic_slice_in_dim(keyval_all, (kv_count + shared_head) * HD, HD, 1)
    q_rot = rotate(queries.reshape(pack_len, HQ_DEV, HD), position, HD).astype(jnp.bfloat16)
    k_rot = rotate(keys.astype(jnp.float32)[:, None, :], position, HD)[:, 0, :].astype(jnp.bfloat16)
    scores = jnp.einsum(
        "qhd,kd->hqk", q_rot, k_rot, preferred_element_type=jnp.float32
    ) / math.sqrt(HD)
    places = jnp.arange(pack_len, dtype=jnp.int32)
    allowed = (doc_id[:, None] == doc_id[None, :]) & (places[None, :] <= places[:, None])
    masked = jnp.where(allowed[None], scores, -jnp.inf)
    row_max = jnp.max(masked, axis=2, keepdims=True)
    exponent = jnp.exp(masked - row_max)
    weights = (exponent / jnp.sum(exponent, axis=2, keepdims=True)).astype(jnp.bfloat16)
    context = jnp.einsum("hqk,kd->qhd", weights, values, preferred_element_type=jnp.float32)
    context = context.astype(jnp.bfloat16).reshape(pack_len, HQ_DEV * HD)
    partial_sum = jnp.dot(context, out_weight, preferred_element_type=jnp.float32)
    summed = lax.psum_scatter(
        partial_sum.astype(jnp.bfloat16), "tensor", scatter_dimension=1, tiled=True
    ).astype(jnp.float32)
    result = jnp.where(is_valid[:, None], summed + packed.astype(jnp.float32), 0.0)
    return result.astype(jnp.bfloat16)


MESH = pl.DeviceIdType.MESH
CORES = 2
HALO = 16


def aligned(index, size):
    return pl.multiple_of(index * size, size)


def fused_kernel(
    cfg, pk_col, pk_row, len_col, len_row, gain, cos_tab, sin_tab, roll_in, w_in, o_in, out,
    wbuf, obuf, sendb, recvb, packed, scaled, q_part, kv_part, kv_acc, q_recv, kv_recv, ctx,
    pos_buf, valid_buf, send_sems, recv_sems, local_sems,
):
    n_dp, n_t, length, feat, per_source = cfg
    chips = n_dp // CORES
    w_sub = wbuf.shape[1] // n_dp
    o_rows = o_in.shape[0]
    o_sub = o_rows // n_dp
    block = length // n_dp
    most = length // per_source
    rows = length // n_t
    qd = w_in.shape[2]
    quarter = feat // 4
    me = lax.axis_index("dp")
    t = lax.axis_index("tensor")
    core = lax.rem(me, CORES)
    chip = lax.div(me, CORES)
    partner = chip * CORES + (CORES - 1 - core)

    def t_at(k):
        return lax.rem(t + k, n_t)

    def chip_at(k):
        return lax.rem(chip + k, chips) * CORES + core

    barrier = pltpu.get_barrier_semaphore()
    for k in range(1, n_dp):
        pl.semaphore_signal(
            barrier, inc=1, device_id=(lax.rem(me + k, n_dp), t), device_id_type=MESH
        )
    for k in range(1, n_t):
        pl.semaphore_signal(barrier, inc=1, device_id=(me, t_at(k)), device_id_type=MESH)
    pl.semaphore_wait(barrier, n_dp + n_t - 2)

    started = []

    def send(source, target, device):
        at = len(started)
        copy = pltpu.make_async_remote_copy(
            src_ref=source,
            dst_ref=target,
            send_sem=send_sems.at[at],
            recv_sem=recv_sems.at[at],
            device_id=device,
            device_id_type=MESH,
        )
        copy.start()
        started.append(copy)
        return copy

    w_first, o_first = {}, {}
    for k in range(1, n_t):
        to = t_at(k)
        w_first[k] = send(
            w_in.at[to, pl.ds(aligned(me, w_sub), w_sub)],
            wbuf.at[t, pl.ds(aligned(me, w_sub), w_sub)],
            (me, to),
        )
    own_w = pltpu.make_async_copy(w_in.at[t], wbuf.at[t], local_sems.at[0])
    own_w.start()
    for k in range(1, n_t):
        to = t_at(k)
        o_first[k] = send(
            o_in.at[pl.ds(aligned(me, o_sub), o_sub), pl.ds(aligned(to, feat), feat)],
            obuf.at[t, pl.ds(aligned(me, o_sub), o_sub)],
            (me, to),
        )
    own_o = pltpu.make_async_copy(
        o_in.at[:, pl.ds(aligned(t, feat), feat)], obuf.at[t], local_sems.at[1]
    )
    own_o.start()

    down = lax.broadcasted_iota(jnp.int32, (length, length), 0).astype(jnp.float32)
    across = lax.broadcasted_iota(jnp.int32, (length, length), 1).astype(jnp.float32)

    def part(value, size):
        return jnp.floor((value + 0.5) * (1.0 / size))

    def pick(mask, value, axis):
        return jnp.sum(jnp.where(mask, value, 0.0), axis=axis, keepdims=True)

    same = part(down, per_source) == part(across, per_source)
    len_c, len_r = len_col[...], len_row[...]
    pk_c, pk_r = pk_col[...], pk_row[...]
    src_start = pick(same & (across < down), len_r, 1)
    chosen = down == pk_r
    q_len_r = pick(chosen, len_c, 0)
    q_start_r = pick(chosen, src_start, 0)
    q_len_c = pick(across == pk_c, len_r, 1)
    earlier = same & (down < across)
    doc_start_r = pick(earlier, q_len_c, 0)
    q_src_r = part(pk_r, per_source)
    slot_r = pick(earlier & (part(pk_c, per_source) == q_src_r), 1.0, 0)
    mine = me.astype(jnp.float32)
    across_1 = across[:1]
    down_1 = down[:, :1]
    owner_r = part(across_1, per_source)
    target = jnp.where(q_src_r == mine, owner_r * (per_source // n_dp) + slot_r, -1.0)
    group = part(down_1, most)
    match = target == group
    token = down_1 - group * most
    row_sent = jnp.where(token < pick(match, q_len_r, 1), pick(match, q_start_r, 1) + token, -1.0)
    take_send = (across == row_sent).astype(jnp.float32).astype(jnp.bfloat16)
    inside = (owner_r == mine) & (doc_start_r <= down) & (down < doc_start_r + q_len_r)
    is_valid = pick(inside, 1.0, 1)
    position = (down_1 - pick(inside, doc_start_r, 1)) * is_valid
    row_got = jnp.where(
        is_valid > 0.0, pick(inside, q_src_r * block + slot_r * most, 1) + position, -1.0
    )
    take_recv = (across == row_got).astype(jnp.float32).astype(jnp.bfloat16)
    pos_buf[:HALO, :] = jnp.zeros((HALO, HD), jnp.float32)
    pos_buf[HALO:, :] = jnp.broadcast_to(position, (length, HD))
    valid_buf[...] = jnp.broadcast_to(is_valid, (length, HD))

    tile = 256
    tiles = feat // tile

    def send_tile(i, carry):
        at = pl.ds(aligned(i, tile), tile)
        sendb[:, at] = jnp.dot(
            take_send, roll_in[:, at], preferred_element_type=jnp.float32
        ).astype(jnp.bfloat16)
        return carry

    lax.fori_loop(0, tiles, send_tile, 0)

    rows_of = {}
    for k in range(1, n_dp):
        to = lax.rem(me + k, n_dp)
        rows_of[k] = send(
            sendb.at[pl.ds(aligned(to, block), block)],
            recvb.at[pl.ds(aligned(me, block), block)],
            (to, t),
        )
    keep = pl.ds(aligned(me, block), block)
    recvb[keep, :] = sendb[keep, :]

    def spread(buf, first, sub):
        hops = {}
        for j in range(1, n_t):
            first[j].wait_recv()
            at = buf.at[t_at(n_t - j), pl.ds(aligned(me, sub), sub)]
            for k in range(1, chips):
                hops[j, k] = send(at, at, (chip_at(k), t))
        return hops

    def share(buf, hops, sub):
        last = []
        for k in range(chips):
            for j in range(1, n_t):
                if k:
                    hops[j, k].wait_recv()
                at = buf.at[
                    t_at(n_t - j), pl.ds(aligned(chip_at(chips - k if k else 0), sub), sub)
                ]
                last.append(send(at, at, (partner, t)))
        return last

    w_hops = spread(wbuf, w_first, w_sub)

    for k in range(1, n_dp):
        rows_of[k].wait_recv()

    def pack_tile(i, total):
        at = pl.ds(aligned(i, tile), tile)
        x = jnp.dot(take_recv, recvb[:, at], preferred_element_type=jnp.float32)
        packed[:, at] = x.astype(jnp.bfloat16)
        g = gain[:, pl.ds(pl.multiple_of(t * feat + i * tile, tile), tile)]
        scaled[:, at] = (x * g).astype(jnp.bfloat16)
        return total + jnp.sum(x * x, axis=1, keepdims=True)

    squares = lax.fori_loop(0, tiles, pack_tile, jnp.zeros((length, 1), jnp.float32))
    lane = lax.broadcasted_iota(jnp.int32, (length, HD), 1)
    high = squares.astype(jnp.bfloat16).astype(jnp.float32)
    kv_part[:HALO, :] = jnp.zeros((HALO, 3 * HD), jnp.bfloat16)
    kv_part[HALO:, 2 * HD :] = jnp.where(
        lane < HD // 2, jnp.broadcast_to(high, (length, HD)), jnp.broadcast_to(squares - high, (length, HD))
    ).astype(jnp.bfloat16)

    o_hops = spread(obuf, o_first, o_sub)
    w_last = share(wbuf, w_hops, w_sub)
    own_w.wait()
    for copy in w_last:
        copy.wait_recv()

    def project(u, carry):
        x = scaled[...]
        q_part[:, pl.ds(aligned(u, qd), qd)] = jnp.dot(
            x, wbuf[u, :feat, :], preferred_element_type=jnp.float32
        ).astype(jnp.bfloat16)
        w = wbuf[u, feat:, :]
        y = jnp.dot(x[:, :quarter], w, preferred_element_type=jnp.float32)
        for i in range(1, 4):
            z = jnp.dot(
                x[:, i * quarter : (i + 1) * quarter], w, preferred_element_type=jnp.float32
            )
            y += pltpu.roll(z, qd - i * (qd // 4), 1)
        kv_acc[u] = y[:, :HD]
        return carry

    lax.fori_loop(0, n_t, project, 0)
    for i in range(2):
        kv_part[HALO:, i * HD : (i + 1) * HD] = jnp.where(
            lane < HD // 2, kv_acc[2 * i], pltpu.roll(kv_acc[2 * i + 1], HD // 2, 1)
        ).astype(jnp.bfloat16)

    shares = []
    for k in range(1, n_t):
        to = t_at(k)
        shares.append(
            send(
                kv_part.at[pl.ds(aligned(to, rows), rows + HALO)], kv_recv.at[k - 1], (me, to)
            )
        )
        shares.append(
            send(q_part.at[pl.ds(aligned(to, rows), rows)], q_recv.at[k - 1], (me, to))
        )
    o_last = share(obuf, o_hops, o_sub)

    for copy in shares:
        copy.wait_recv()
    keys_at = pl.ds(aligned(t, rows), rows + HALO)
    queries_at = pl.ds(aligned(t, rows), rows)
    kv = kv_part[keys_at, :].astype(jnp.float32)
    for k in range(n_t - 1):
        kv += kv_recv[k].astype(jnp.float32)
    sums = jnp.sum(kv[:, 2 * HD :], axis=1, keepdims=True) * (2.0 / HD)
    inverse = lax.rsqrt(sums / (feat * n_t) + epsilon)
    kv_bf = (kv[:, : 2 * HD] * inverse).astype(jnp.bfloat16)
    values = kv_bf[:, HD:]
    pos = pos_buf[keys_at, :]
    cosine = jnp.zeros((rows + HALO, HD), jnp.float32)
    sine = jnp.zeros((rows + HALO, HD), jnp.float32)
    for m in range(most):
        at_m = pos == float(m)
        cosine = jnp.where(at_m, cos_tab[m : m + 1, :], cosine)
        sine = jnp.where(at_m, sin_tab[m : m + 1, :], sine)

    def turn(v, c, s):
        return v * c + pltpu.roll(v, HD // 2, 1) * s

    k_rot = turn(kv_bf[:, :HD].astype(jnp.float32), cosine, sine).astype(jnp.bfloat16)
    q_down = lax.broadcasted_iota(jnp.int32, (rows, rows + HALO), 0).astype(jnp.float32)
    k_across = lax.broadcasted_iota(jnp.int32, (rows, rows + HALO), 1).astype(jnp.float32) - HALO
    allowed = (k_across <= q_down) & (k_across >= q_down - pos[HALO:, :1])
    for h in range(q_part.shape[1] // HD):
        cols = slice(h * HD, (h + 1) * HD)
        q = q_part[queries_at, cols].astype(jnp.float32)
        for k in range(n_t - 1):
            q += q_recv[k, :, cols].astype(jnp.float32)
        q_rot = turn(q * inverse[HALO:], cosine[HALO:], sine[HALO:]).astype(jnp.bfloat16)
        scores = lax.dot_general(
            q_rot, k_rot, (((1,), (1,)), ((), ())), preferred_element_type=jnp.float32
        ) * (1.0 / math.sqrt(HD))
        scores = jnp.where(allowed, scores, -jnp.inf)
        exponent = jnp.exp(scores - jnp.max(scores, axis=1, keepdims=True))
        weights = (exponent / jnp.sum(exponent, axis=1, keepdims=True)).astype(jnp.bfloat16)
        ctx[queries_at, cols] = jnp.dot(
            weights, values, preferred_element_type=jnp.float32
        ).astype(jnp.bfloat16)

    gathers = []
    for k in range(1, n_t):
        at = ctx.at[queries_at]
        gathers.append(send(at, at, (me, t_at(k))))
    own_o.wait()
    for copy in o_last:
        copy.wait_recv()
    for copy in gathers:
        copy.wait_recv()

    def out_tile(i, carry):
        at = pl.ds(aligned(i, tile), tile)
        total = packed[:, at].astype(jnp.float32)
        for u in range(n_t):
            total += jnp.dot(
                ctx[:, u * o_rows : (u + 1) * o_rows],
                obuf[u, :, at],
                preferred_element_type=jnp.float32,
            )
        out[:, at] = jnp.where(valid_buf[:, :1] > 0.0, total, 0.0).astype(jnp.bfloat16)
        return carry

    lax.fori_loop(0, tiles, out_tile, 0)
    for copy in started:
        copy.wait_send()


def fused_body(rollout, lengths, packing, norm_gain, query_weight, keyval_weight, out_weight):
    n_dp, n_t = lax.axis_size("dp"), lax.axis_size("tensor")
    length, feat = rollout.shape
    per_source = lengths.shape[1]
    most = length // per_source
    qd, kd = query_weight.shape[1], keyval_weight.shape[1]
    quarter = feat // 4
    kv = keyval_weight.reshape(n_t, 4, quarter, kd)
    w = jnp.concatenate(
        [query_weight.reshape(n_t, feat, qd), jnp.concatenate([kv[:, i] for i in range(4)], axis=2)],
        axis=1,
    )
    pk = packing.astype(jnp.float32)
    flat = lengths.reshape(-1).astype(jnp.float32)
    frequency = np.float32(rope_base) ** (-np.arange(HD // 2, dtype=np.float32) * 2.0 / HD)
    angles = np.arange(most, dtype=np.float32)[:, None] * frequency[None, :].astype(np.float32)
    cos_tab = np.concatenate([np.cos(angles)] * 2, axis=1).astype(np.float32)
    sin_tab = np.concatenate([-np.sin(angles), np.sin(angles)], axis=1).astype(np.float32)
    rows = length // n_t
    chips = n_dp // CORES
    copies = 2 * (n_t - 1) * (1 + chips - 1 + chips) + (n_dp - 1) + 3 * (n_t - 1)
    vmem = pl.BlockSpec(memory_space=pltpu.VMEM)
    hbm = pl.BlockSpec(memory_space=pl.ANY)
    bf, f32 = jnp.bfloat16, jnp.float32
    return pl.pallas_call(
        functools.partial(fused_kernel, (n_dp, n_t, length, feat, per_source)),
        out_shape=jax.ShapeDtypeStruct((length, feat), bf),
        in_specs=[vmem] * 8 + [hbm] * 2,
        out_specs=vmem,
        scratch_shapes=[
            pltpu.VMEM(w.shape, bf),
            pltpu.VMEM((n_t, out_weight.shape[0], feat), bf),
            pltpu.VMEM((length, feat), bf),
            pltpu.VMEM((length, feat), bf),
            pltpu.VMEM((length, feat), bf),
            pltpu.VMEM((length, feat), bf),
            pltpu.VMEM((length, n_t * qd), bf),
            pltpu.VMEM((length + HALO, 3 * HD), bf),
            pltpu.VMEM((n_t, length, HD), f32),
            pltpu.VMEM((n_t - 1, rows, n_t * qd), bf),
            pltpu.VMEM((n_t - 1, rows + HALO, 3 * HD), bf),
            pltpu.VMEM((length, n_t * qd), bf),
            pltpu.VMEM((length + HALO, HD), f32),
            pltpu.VMEM((length, HD), f32),
            pltpu.SemaphoreType.DMA((copies,)),
            pltpu.SemaphoreType.DMA((copies,)),
            pltpu.SemaphoreType.DMA((2,)),
        ],
        compiler_params=pltpu.CompilerParams(
            collective_id=0, has_side_effects=True, vmem_limit_bytes=48 * 1024 * 1024
        ),
    )(
        pk[:, None], pk[None, :], flat[:, None], flat[None, :], norm_gain[None, :],
        jnp.asarray(cos_tab), jnp.asarray(sin_tab), rollout, w, out_weight,
    )


def body(rollout, lengths, packing, norm_gain, query_weight, keyval_weight, out_weight):
    n_dp, n_t = lax.axis_size("dp"), lax.axis_size("tensor")
    length, feat = rollout.shape
    qd, kd = query_weight.shape[1], keyval_weight.shape[1]
    fits = (
        kd * n_t == 2 * HD
        and n_t == 4
        and qd == 4 * kd
        and n_dp % CORES == 0
        and length % (n_t * HALO) == 0
        and packing.shape[0] == length
        and (length // n_dp) % HALO == 0
        and feat % 512 == 0
        and lengths.shape[1] % n_dp == 0
    )
    chosen = fused_body if fits else plain_body
    return chosen(rollout, lengths, packing, norm_gain, query_weight, keyval_weight, out_weight)


def solution(mesh):
    in_specs = (
        P("dp", "tensor"),
        P(),
        P(),
        P(),
        P(None, "tensor"),
        P(None, "tensor"),
        P("tensor", None),
    )
    out_specs = P("dp", "tensor")
    return jax.shard_map(body, mesh=mesh, in_specs=in_specs, out_specs=out_specs, check_vma=False)
```

```python
import functools
import math

import numpy as np
import jax
import jax.numpy as jnp
from jax import lax
from jax.experimental import pallas as pl
from jax.experimental.pallas import tpu as pltpu
from jax.sharding import PartitionSpec as P

D = 6144
HD = 128
HQ_DEV = 2
GROUP = 8


epsilon = 1e-05
rope_base = 500000.0


def owner_map(lengths, packing, owner_id, pack_len):
    per_source = lengths.shape[1]
    chosen = lax.dynamic_slice_in_dim(packing, owner_id * per_source, per_source)
    ordered = jnp.take(lengths.reshape(-1), chosen)
    doc_start = jnp.cumsum(ordered) - ordered
    places = jnp.arange(pack_len, dtype=jnp.int32)
    inside = (places[:, None] >= doc_start[None, :]) & (
        places[:, None] < (doc_start + ordered)[None, :]
    )
    is_valid = jnp.any(inside, axis=1)
    slot_of = jnp.sum(
        jnp.where(inside, jnp.arange(per_source, dtype=jnp.int32)[None, :], 0), axis=1
    )
    response = jnp.take(chosen, slot_of)
    position = jnp.where(is_valid, places - jnp.take(doc_start, slot_of), 0)
    doc_id = jnp.where(is_valid, slot_of, per_source)
    return (response, position, doc_id, is_valid)


def rotate(values, position, head_dim):
    half_dim = head_dim // 2
    frequency = rope_base ** (-jnp.arange(half_dim, dtype=jnp.float32) * 2.0 / head_dim)
    angles = position.astype(jnp.float32)[:, None] * frequency[None, :]
    cosine = jnp.concatenate([jnp.cos(angles), jnp.cos(angles)], axis=1)[:, None, :]
    sine_table = jnp.concatenate([jnp.sin(angles), jnp.sin(angles)], axis=1)[:, None, :]
    turned = jnp.concatenate([-values[..., half_dim:], values[..., :half_dim]], axis=-1)
    return values * cosine + turned * sine_table


def plain_body(rollout, lengths, packing, norm_gain, query_weight, keyval_weight, out_weight):
    owner_id = lax.axis_index("dp")
    tensor_index = lax.axis_index("tensor")
    tensor_count = lax.axis_size("tensor")
    pack_len = rollout.shape[0]
    per_source = lengths.shape[1]
    response, position, doc_id, is_valid = owner_map(lengths, packing, owner_id, pack_len)
    source_start = jnp.cumsum(lengths, axis=1) - lengths
    global_row = (
        response // per_source * pack_len + jnp.take(source_start.reshape(-1), response) + position
    )
    portion = lax.all_gather(rollout, "dp", axis=0, tiled=True)
    within = is_valid & (global_row >= 0) & (global_row < portion.shape[0])
    picked = jnp.take(portion, jnp.clip(global_row, 0, portion.shape[0] - 1), axis=0)
    packed = jnp.where(within[:, None], picked, jnp.zeros_like(rollout))
    widened = lax.all_gather(packed, "tensor", axis=1, tiled=True).astype(jnp.float32)
    scaled = (widened * norm_gain[None, :]).astype(jnp.bfloat16)
    query_acc = jnp.dot(scaled, query_weight, preferred_element_type=jnp.float32)
    keyval_acc = jnp.dot(scaled, keyval_weight, preferred_element_type=jnp.float32)
    squares = jnp.sum(widened * widened, axis=1)
    query_acc, keyval_acc, squares = (query_acc, keyval_acc, squares)
    inverse = lax.rsqrt(squares / D + epsilon)
    queries = query_acc * inverse[:, None]
    keyval_share = (keyval_acc * inverse[:, None]).astype(jnp.bfloat16)
    keyval_all = lax.all_gather(keyval_share, "tensor", axis=1, tiled=True)
    kv_count = keyval_weight.shape[1] * tensor_count // (2 * HD)
    shared_head = tensor_index * HQ_DEV // GROUP
    keys = lax.dynamic_slice_in_dim(keyval_all, shared_head * HD, HD, 1)
    values = lax.dynamic_slice_in_dim(keyval_all, (kv_count + shared_head) * HD, HD, 1)
    q_rot = rotate(queries.reshape(pack_len, HQ_DEV, HD), position, HD).astype(jnp.bfloat16)
    k_rot = rotate(keys.astype(jnp.float32)[:, None, :], position, HD)[:, 0, :].astype(jnp.bfloat16)
    scores = jnp.einsum(
        "qhd,kd->hqk", q_rot, k_rot, preferred_element_type=jnp.float32
    ) / math.sqrt(HD)
    places = jnp.arange(pack_len, dtype=jnp.int32)
    allowed = (doc_id[:, None] == doc_id[None, :]) & (places[None, :] <= places[:, None])
    masked = jnp.where(allowed[None], scores, -jnp.inf)
    row_max = jnp.max(masked, axis=2, keepdims=True)
    exponent = jnp.exp(masked - row_max)
    weights = (exponent / jnp.sum(exponent, axis=2, keepdims=True)).astype(jnp.bfloat16)
    context = jnp.einsum("hqk,kd->qhd", weights, values, preferred_element_type=jnp.float32)
    context = context.astype(jnp.bfloat16).reshape(pack_len, HQ_DEV * HD)
    partial_sum = jnp.dot(context, out_weight, preferred_element_type=jnp.float32)
    summed = lax.psum_scatter(
        partial_sum.astype(jnp.bfloat16), "tensor", scatter_dimension=1, tiled=True
    ).astype(jnp.float32)
    result = jnp.where(is_valid[:, None], summed + packed.astype(jnp.float32), 0.0)
    return result.astype(jnp.bfloat16)


MESH = pl.DeviceIdType.MESH
CORES = 2
HALO = 16


def aligned(index, size):
    return pl.multiple_of(index * size, size)


def fused_kernel(
    cfg, pk_hbm, len_hbm, gain_hbm, tab_hbm, roll_hbm, w_in, k_in, o_in, out,
    pk_buf, len_buf, gain, tab, wbuf, kbuf, obuf, roll_in, sendb, recvb, packed, scaled, q_part, kv_part, q_recv, kv_recv, ctx,
    pos_buf, valid_buf, send_sems, recv_sems, local_sems,
):
    n_dp, n_t, length, feat, per_source = cfg
    chips = n_dp // CORES
    w_sub = feat // n_dp
    kd = k_in.shape[0]
    k_rows, k_cols = kd // chips, feat // CORES
    o_rows = o_in.shape[0]
    o_sub = o_rows // n_dp
    block = length // n_dp
    most = length // per_source
    rows = length // n_t
    qd = w_in.shape[1]
    me = lax.axis_index("dp")
    t = lax.axis_index("tensor")
    core = lax.rem(me, CORES)
    chip = lax.div(me, CORES)
    partner = chip * CORES + (CORES - 1 - core)

    def t_at(k):
        return lax.rem(t + k, n_t)

    def chip_at(k):
        return lax.rem(chip + k, chips) * CORES + core

    small = [
        pltpu.make_async_copy(source, target, local_sems.at[4 + i])
        for i, (source, target) in enumerate(
            (
                (pk_hbm, pk_buf),
                (len_hbm, len_buf),
                (gain_hbm.at[:, pl.ds(aligned(t, feat), feat)], gain),
                (tab_hbm, tab),
            )
        )
    ]
    load = pltpu.make_async_copy(roll_hbm, roll_in, local_sems.at[2])
    for copy in [*small, load]:
        copy.start()

    barrier = pltpu.get_barrier_semaphore()
    for k in range(1, n_dp):
        pl.semaphore_signal(
            barrier, inc=1, device_id=(lax.rem(me + k, n_dp), t), device_id_type=MESH
        )
    for k in range(1, n_t):
        pl.semaphore_signal(barrier, inc=1, device_id=(me, t_at(k)), device_id_type=MESH)
    pl.semaphore_wait(barrier, n_dp + n_t - 2)

    started = []

    def send(source, target, device):
        at = len(started)
        copy = pltpu.make_async_remote_copy(
            src_ref=source,
            dst_ref=target,
            send_sem=send_sems.at[at],
            recv_sem=recv_sems.at[at],
            device_id=device,
            device_id_type=MESH,
        )
        copy.start()
        started.append(copy)
        return copy

    def w_at(u, h, c):
        return wbuf.at[u, pl.ds(aligned(h * CORES + c, w_sub), w_sub)]

    def k_at(u, h, c):
        return kbuf.at[
            pl.ds(aligned(u * chips + h, k_rows), k_rows), pl.ds(aligned(c, k_cols), k_cols)
        ]

    def o_at(u, h, c):
        return obuf.at[u, pl.ds(aligned(h * CORES + c, o_sub), o_sub)]

    w_first, k_first, o_first = {}, {}, {}
    for k in range(1, n_t):
        to = t_at(k)
        k_first[k] = send(
            k_in.at[
                pl.ds(aligned(chip, k_rows), k_rows),
                pl.ds(aligned(to * CORES + core, k_cols), k_cols),
            ],
            k_at(t, chip, core),
            (me, to),
        )
    for k in range(1, n_t):
        to = t_at(k)
        w_first[k] = send(
            w_in.at[pl.ds(aligned(to * n_dp + me, w_sub), w_sub)], w_at(t, chip, core), (me, to)
        )
    own_w = pltpu.make_async_copy(
        w_in.at[pl.ds(aligned(t, feat), feat)], wbuf.at[t], local_sems.at[0]
    )
    own_w.start()
    own_k = pltpu.make_async_copy(
        k_in.at[:, pl.ds(aligned(t, feat), feat)],
        kbuf.at[pl.ds(aligned(t, kd), kd)],
        local_sems.at[3],
    )
    own_k.start()
    for k in range(1, n_t):
        to = t_at(k)
        o_first[k] = send(
            o_in.at[pl.ds(aligned(me, o_sub), o_sub), pl.ds(aligned(to, feat), feat)],
            o_at(t, chip, core),
            (me, to),
        )
    own_o = pltpu.make_async_copy(
        o_in.at[:, pl.ds(aligned(t, feat), feat)], obuf.at[t], local_sems.at[1]
    )
    own_o.start()

    down = lax.broadcasted_iota(jnp.int32, (length, length), 0).astype(jnp.float32)
    across = lax.broadcasted_iota(jnp.int32, (length, length), 1).astype(jnp.float32)

    def part(value, size):
        return jnp.floor((value + 0.5) * (1.0 / size))

    def pick(mask, value, axis):
        return jnp.sum(jnp.where(mask, value, 0.0), axis=axis, keepdims=True)

    same = part(down, per_source) == part(across, per_source)
    diagonal = down == across
    for copy in small:
        copy.wait()
    len_all = len_buf[...].astype(jnp.float32)
    source_of = part(down[:, :1], per_source)
    table = jnp.zeros((length, per_source), jnp.float32)
    for i in range(n_dp):
        table = jnp.where(source_of == float(i), len_all[i : i + 1, :], table)
    within = down[:, :per_source] - source_of * per_source
    len_c = pick(across[:, :per_source] == within, table, 1)
    len_r = pick(diagonal, len_c, 0)
    pk_r = pk_buf[...].astype(jnp.float32)
    pk_c = pick(diagonal, pk_r, 1)
    src_start = pick(same & (across < down), len_r, 1)
    chosen = down == pk_r
    q_len_r = pick(chosen, len_c, 0)
    q_start_r = pick(chosen, src_start, 0)
    q_len_c = pick(across == pk_c, len_r, 1)
    earlier = same & (down < across)
    doc_start_r = pick(earlier, q_len_c, 0)
    q_src_r = part(pk_r, per_source)
    slot_r = pick(earlier & (part(pk_c, per_source) == q_src_r), 1.0, 0)
    mine = me.astype(jnp.float32)
    across_1 = across[:1]
    down_1 = down[:, :1]
    owner_r = part(across_1, per_source)
    target = jnp.where(q_src_r == mine, owner_r * (per_source // n_dp) + slot_r, -1.0)
    group = part(down_1, most)
    match = target == group
    token = down_1 - group * most
    row_sent = jnp.where(token < pick(match, q_len_r, 1), pick(match, q_start_r, 1) + token, -1.0)
    take_send = (across == row_sent).astype(jnp.float32).astype(jnp.bfloat16)
    inside = (owner_r == mine) & (doc_start_r <= down) & (down < doc_start_r + q_len_r)
    is_valid = pick(inside, 1.0, 1)
    position = (down_1 - pick(inside, doc_start_r, 1)) * is_valid
    row_got = jnp.where(
        is_valid > 0.0, pick(inside, q_src_r * block + slot_r * most, 1) + position, -1.0
    )
    take_recv = (across == row_got).astype(jnp.float32).astype(jnp.bfloat16)
    pos_buf[:HALO, :] = jnp.zeros((HALO, HD), jnp.float32)
    pos_buf[HALO:, :] = jnp.broadcast_to(position, (length, HD))
    valid_buf[...] = jnp.broadcast_to(is_valid, (length, HD))

    tile = 256
    tiles = feat // tile

    def send_tile(i, carry):
        at = pl.ds(aligned(i, tile), tile)
        sendb[:, at] = jnp.dot(
            take_send, roll_in[:, at], preferred_element_type=jnp.float32
        ).astype(jnp.bfloat16)
        return carry

    load.wait()
    lax.fori_loop(0, tiles, send_tile, 0)

    rows_of = {}
    for k in range(1, n_dp):
        to = lax.rem(me + k, n_dp)
        rows_of[k] = send(
            sendb.at[pl.ds(aligned(to, block), block)],
            recvb.at[pl.ds(aligned(me, block), block)],
            (to, t),
        )
    keep = pl.ds(aligned(me, block), block)
    recvb[keep, :] = sendb[keep, :]

    def spread(at, first, j):
        first[j].wait_recv()
        ref = at(t_at(n_t - j), chip, core)
        return [send(ref, ref, (chip_at(k), t)) for k in range(1, chips)]

    def share(at, hops, j):
        last = []
        for k in range(chips):
            if k:
                hops[k - 1].wait_recv()
            ref = at(t_at(n_t - j), lax.rem(chip + chips - k, chips), core)
            last.append(send(ref, ref, (partner, t)))
        return last

    others = range(1, n_t)
    k_hops = {j: spread(k_at, k_first, j) for j in others}
    w_hops = {1: spread(w_at, w_first, 1)}

    for k in range(1, n_dp):
        rows_of[k].wait_recv()

    def pack_tile(i, total):
        at = pl.ds(aligned(i, tile), tile)
        x = jnp.dot(take_recv, recvb[:, at], preferred_element_type=jnp.float32)
        packed[:, at] = x.astype(jnp.bfloat16)
        g = gain[:, at]
        scaled[:, at] = (x * g).astype(jnp.bfloat16)
        return total + jnp.sum(x * x, axis=1, keepdims=True)

    squares = lax.fori_loop(0, tiles, pack_tile, jnp.zeros((length, 1), jnp.float32))
    lane = lax.broadcasted_iota(jnp.int32, (length, HD), 1)
    high = squares.astype(jnp.bfloat16).astype(jnp.float32)
    kv_part[:HALO, :] = jnp.zeros((HALO, 3 * HD), jnp.bfloat16)
    kv_part[HALO:, 2 * HD :] = jnp.where(
        lane < HD // 2, jnp.broadcast_to(high, (length, HD)), jnp.broadcast_to(squares - high, (length, HD))
    ).astype(jnp.bfloat16)

    shares = []

    def reduce_rows(part_ref, recv_ref, extra, cols):
        for k in others:
            to = t_at(k)
            shares.append(
                send(
                    part_ref.at[pl.ds(aligned(to, rows), rows + extra), cols],
                    recv_ref.at[k - 1, :, cols],
                    (me, to),
                )
            )

    def project(j):
        u = t_at(n_t - j)
        cols = pl.ds(aligned(u, qd), qd)
        q_part[:, cols] = jnp.dot(
            scaled[...], wbuf[u], preferred_element_type=jnp.float32
        ).astype(jnp.bfloat16)
        reduce_rows(q_part, q_recv, 0, cols)

    own_w.wait()
    own_k.wait()
    reduce_rows(kv_part, kv_recv, HALO, pl.ds(2 * HD, HD))
    project(n_t)
    for j in others[1:]:
        w_hops[j] = spread(w_at, w_first, j)
    k_last = [copy for j in others for copy in share(k_at, k_hops[j], j)]
    for copy in k_last:
        copy.wait_recv()
    kv_part[HALO:, : 2 * HD] = lax.dot_general(
        scaled[...], kbuf[...], (((1,), (1,)), ((), ())), preferred_element_type=jnp.float32
    ).astype(jnp.bfloat16)
    reduce_rows(kv_part, kv_recv, HALO, pl.ds(0, 2 * HD))
    w_last = share(w_at, w_hops[1], 1)
    o_hops = {}
    for j in others:
        if j + 1 in w_hops:
            following = share(w_at, w_hops[j + 1], j + 1)
        for copy in w_last:
            copy.wait_recv()
        w_last = following
        project(j)
        o_hops[j] = spread(o_at, o_first, j)
    for copy in shares:
        copy.wait_recv()

    keys_at = pl.ds(aligned(t, rows), rows + HALO)
    queries_at = pl.ds(aligned(t, rows), rows)
    kv = kv_part[keys_at, :].astype(jnp.float32)
    for k in range(n_t - 1):
        kv += kv_recv[k].astype(jnp.float32)
    sums = jnp.sum(kv[:, 2 * HD :], axis=1, keepdims=True) * (2.0 / HD)
    inverse = lax.rsqrt(sums / (feat * n_t) + epsilon)
    kv_bf = (kv[:, : 2 * HD] * inverse).astype(jnp.bfloat16)
    values = kv_bf[:, HD:]
    pos = pos_buf[keys_at, :]
    cosine = jnp.zeros((rows + HALO, HD), jnp.float32)
    sine = jnp.zeros((rows + HALO, HD), jnp.float32)
    for m in range(most):
        at_m = pos == float(m)
        cosine = jnp.where(at_m, tab[m : m + 1, :], cosine)
        sine = jnp.where(at_m, tab[most + m : most + m + 1, :], sine)

    def turn(v, c, s):
        return v * c + pltpu.roll(v, HD // 2, 1) * s

    k_rot = turn(kv_bf[:, :HD].astype(jnp.float32), cosine, sine).astype(jnp.bfloat16)
    q_down = lax.broadcasted_iota(jnp.int32, (rows, rows + HALO), 0).astype(jnp.float32)
    k_across = lax.broadcasted_iota(jnp.int32, (rows, rows + HALO), 1).astype(jnp.float32) - HALO
    allowed = (k_across <= q_down) & (k_across >= q_down - pos[HALO:, :1])
    gathers = []
    heads = q_part.shape[1] // HD
    for h in range(heads):
        cols = slice(h * HD, (h + 1) * HD)
        q = q_part[queries_at, cols].astype(jnp.float32)
        for k in range(n_t - 1):
            q += q_recv[k, :, cols].astype(jnp.float32)
        q_rot = turn(q * inverse[HALO:], cosine[HALO:], sine[HALO:]).astype(jnp.bfloat16)
        scores = lax.dot_general(
            q_rot, k_rot, (((1,), (1,)), ((), ())), preferred_element_type=jnp.float32
        ) * (1.0 / math.sqrt(HD))
        scores = jnp.where(allowed, scores, -jnp.inf)
        exponent = jnp.exp(scores - jnp.max(scores, axis=1, keepdims=True))
        weights = (exponent / jnp.sum(exponent, axis=1, keepdims=True)).astype(jnp.bfloat16)
        ctx[queries_at, cols] = jnp.dot(
            weights, values, preferred_element_type=jnp.float32
        ).astype(jnp.bfloat16)
        if (h + 1) % (heads // n_t) == 0:
            at = ctx.at[queries_at, pl.ds((h + 1 - heads // n_t) * HD, heads // n_t * HD)]
            for k in others:
                gathers.append(send(at, at, (me, t_at(k))))

    o_last = [copy for j in others for copy in share(o_at, o_hops[j], j)]
    own_o.wait()
    for copy in o_last:
        copy.wait_recv()
    for copy in gathers:
        copy.wait_recv()

    def out_tile(i, carry):
        at = pl.ds(aligned(i, tile), tile)
        total = packed[:, at].astype(jnp.float32)
        for u in range(n_t):
            total += jnp.dot(
                ctx[:, u * o_rows : (u + 1) * o_rows],
                obuf[u, :, at],
                preferred_element_type=jnp.float32,
            )
        out[:, at] = jnp.where(valid_buf[:, :1] > 0.0, total, 0.0).astype(jnp.bfloat16)
        return carry

    lax.fori_loop(0, tiles, out_tile, 0)
    for copy in started:
        copy.wait_send()


def fused_body(rollout, lengths, packing, norm_gain, query_weight, keyval_weight, out_weight):
    n_dp, n_t = lax.axis_size("dp"), lax.axis_size("tensor")
    length, feat = rollout.shape
    per_source = lengths.shape[1]
    most = length // per_source
    qd, kd = query_weight.shape[1], keyval_weight.shape[1]
    frequency = np.float32(rope_base) ** (-np.arange(HD // 2, dtype=np.float32) * 2.0 / HD)
    angles = np.arange(most, dtype=np.float32)[:, None] * frequency[None, :].astype(np.float32)
    cos_tab = np.concatenate([np.cos(angles)] * 2, axis=1).astype(np.float32)
    sin_tab = np.concatenate([-np.sin(angles), np.sin(angles)], axis=1).astype(np.float32)
    rows = length // n_t
    chips = n_dp // CORES
    copies = 3 * (n_t - 1) * (1 + chips - 1 + chips) + (n_dp - 1) + (2 + 2 * n_t) * (n_t - 1)
    vmem = pl.BlockSpec(memory_space=pltpu.VMEM)
    hbm = pl.BlockSpec(memory_space=pl.ANY)
    bf, f32 = jnp.bfloat16, jnp.float32
    return pl.pallas_call(
        functools.partial(fused_kernel, (n_dp, n_t, length, feat, per_source)),
        out_shape=jax.ShapeDtypeStruct((length, feat), bf),
        in_specs=[hbm] * 8,
        out_specs=vmem,
        scratch_shapes=[
            pltpu.VMEM((1, packing.shape[0]), jnp.int32),
            pltpu.VMEM(lengths.shape, jnp.int32),
            pltpu.VMEM((1, feat), f32),
            pltpu.VMEM((2 * most, HD), f32),
            pltpu.VMEM((n_t, feat, qd), bf),
            pltpu.VMEM((n_t * kd, feat), bf),
            pltpu.VMEM((n_t, out_weight.shape[0], feat), bf),
            pltpu.VMEM((length, feat), bf),
            pltpu.VMEM((length, feat), bf),
            pltpu.VMEM((length, feat), bf),
            pltpu.VMEM((length, feat), bf),
            pltpu.VMEM((length, feat), bf),
            pltpu.VMEM((length, n_t * qd), bf),
            pltpu.VMEM((length + HALO, 3 * HD), bf),
            pltpu.VMEM((n_t - 1, rows, n_t * qd), bf),
            pltpu.VMEM((n_t - 1, rows + HALO, 3 * HD), bf),
            pltpu.VMEM((length, n_t * qd), bf),
            pltpu.VMEM((length + HALO, HD), f32),
            pltpu.VMEM((length, HD), f32),
            pltpu.SemaphoreType.DMA((copies,)),
            pltpu.SemaphoreType.DMA((copies,)),
            pltpu.SemaphoreType.DMA((8,)),
        ],
        compiler_params=pltpu.CompilerParams(
            collective_id=0, has_side_effects=True, vmem_limit_bytes=60 * 1024 * 1024
        ),
    )(
        packing[None, :], lengths, norm_gain[None, :],
        jnp.asarray(np.concatenate([cos_tab, sin_tab])), rollout, query_weight,
        keyval_weight.T, out_weight,
    )


def body(rollout, lengths, packing, norm_gain, query_weight, keyval_weight, out_weight):
    n_dp, n_t = lax.axis_size("dp"), lax.axis_size("tensor")
    length, feat = rollout.shape
    qd, kd = query_weight.shape[1], keyval_weight.shape[1]
    fits = (
        kd * n_t == 2 * HD
        and n_t == 4
        and kd % (HALO * n_dp // CORES) == 0
        and feat % (128 * CORES) == 0
        and n_dp % CORES == 0
        and length % (n_t * HALO) == 0
        and packing.shape[0] == length
        and (length // n_dp) % HALO == 0
        and feat % 512 == 0
        and lengths.shape[1] % n_dp == 0
    )
    chosen = fused_body if fits else plain_body
    return chosen(rollout, lengths, packing, norm_gain, query_weight, keyval_weight, out_weight)


def solution(mesh):
    in_specs = (
        P("dp", "tensor"),
        P(),
        P(),
        P(),
        P(None, "tensor"),
        P(None, "tensor"),
        P("tensor", None),
    )
    out_specs = P("dp", "tensor")
    return jax.shard_map(body, mesh=mesh, in_specs=in_specs, out_specs=out_specs, check_vma=False)
```

```python
import functools
import math

import numpy as np
import jax
import jax.numpy as jnp
from jax import lax
from jax.experimental import pallas as pl
from jax.experimental.pallas import tpu as pltpu
from jax.sharding import PartitionSpec as P

D = 6144
HD = 128
HQ_DEV = 2
GROUP = 8


epsilon = 1e-05
rope_base = 500000.0


def owner_map(lengths, packing, owner_id, pack_len):
    per_source = lengths.shape[1]
    chosen = lax.dynamic_slice_in_dim(packing, owner_id * per_source, per_source)
    ordered = jnp.take(lengths.reshape(-1), chosen)
    doc_start = jnp.cumsum(ordered) - ordered
    places = jnp.arange(pack_len, dtype=jnp.int32)
    inside = (places[:, None] >= doc_start[None, :]) & (
        places[:, None] < (doc_start + ordered)[None, :]
    )
    is_valid = jnp.any(inside, axis=1)
    slot_of = jnp.sum(
        jnp.where(inside, jnp.arange(per_source, dtype=jnp.int32)[None, :], 0), axis=1
    )
    response = jnp.take(chosen, slot_of)
    position = jnp.where(is_valid, places - jnp.take(doc_start, slot_of), 0)
    doc_id = jnp.where(is_valid, slot_of, per_source)
    return (response, position, doc_id, is_valid)


def rotate(values, position, head_dim):
    half_dim = head_dim // 2
    frequency = rope_base ** (-jnp.arange(half_dim, dtype=jnp.float32) * 2.0 / head_dim)
    angles = position.astype(jnp.float32)[:, None] * frequency[None, :]
    cosine = jnp.concatenate([jnp.cos(angles), jnp.cos(angles)], axis=1)[:, None, :]
    sine_table = jnp.concatenate([jnp.sin(angles), jnp.sin(angles)], axis=1)[:, None, :]
    turned = jnp.concatenate([-values[..., half_dim:], values[..., :half_dim]], axis=-1)
    return values * cosine + turned * sine_table


def plain_body(rollout, lengths, packing, norm_gain, query_weight, keyval_weight, out_weight):
    owner_id = lax.axis_index("dp")
    tensor_index = lax.axis_index("tensor")
    tensor_count = lax.axis_size("tensor")
    pack_len = rollout.shape[0]
    per_source = lengths.shape[1]
    response, position, doc_id, is_valid = owner_map(lengths, packing, owner_id, pack_len)
    source_start = jnp.cumsum(lengths, axis=1) - lengths
    global_row = (
        response // per_source * pack_len + jnp.take(source_start.reshape(-1), response) + position
    )
    portion = lax.all_gather(rollout, "dp", axis=0, tiled=True)
    within = is_valid & (global_row >= 0) & (global_row < portion.shape[0])
    picked = jnp.take(portion, jnp.clip(global_row, 0, portion.shape[0] - 1), axis=0)
    packed = jnp.where(within[:, None], picked, jnp.zeros_like(rollout))
    widened = lax.all_gather(packed, "tensor", axis=1, tiled=True).astype(jnp.float32)
    scaled = (widened * norm_gain[None, :]).astype(jnp.bfloat16)
    query_acc = jnp.dot(scaled, query_weight, preferred_element_type=jnp.float32)
    keyval_acc = jnp.dot(scaled, keyval_weight, preferred_element_type=jnp.float32)
    squares = jnp.sum(widened * widened, axis=1)
    query_acc, keyval_acc, squares = (query_acc, keyval_acc, squares)
    inverse = lax.rsqrt(squares / D + epsilon)
    queries = query_acc * inverse[:, None]
    keyval_share = (keyval_acc * inverse[:, None]).astype(jnp.bfloat16)
    keyval_all = lax.all_gather(keyval_share, "tensor", axis=1, tiled=True)
    kv_count = keyval_weight.shape[1] * tensor_count // (2 * HD)
    shared_head = tensor_index * HQ_DEV // GROUP
    keys = lax.dynamic_slice_in_dim(keyval_all, shared_head * HD, HD, 1)
    values = lax.dynamic_slice_in_dim(keyval_all, (kv_count + shared_head) * HD, HD, 1)
    q_rot = rotate(queries.reshape(pack_len, HQ_DEV, HD), position, HD).astype(jnp.bfloat16)
    k_rot = rotate(keys.astype(jnp.float32)[:, None, :], position, HD)[:, 0, :].astype(jnp.bfloat16)
    scores = jnp.einsum(
        "qhd,kd->hqk", q_rot, k_rot, preferred_element_type=jnp.float32
    ) / math.sqrt(HD)
    places = jnp.arange(pack_len, dtype=jnp.int32)
    allowed = (doc_id[:, None] == doc_id[None, :]) & (places[None, :] <= places[:, None])
    masked = jnp.where(allowed[None], scores, -jnp.inf)
    row_max = jnp.max(masked, axis=2, keepdims=True)
    exponent = jnp.exp(masked - row_max)
    weights = (exponent / jnp.sum(exponent, axis=2, keepdims=True)).astype(jnp.bfloat16)
    context = jnp.einsum("hqk,kd->qhd", weights, values, preferred_element_type=jnp.float32)
    context = context.astype(jnp.bfloat16).reshape(pack_len, HQ_DEV * HD)
    partial_sum = jnp.dot(context, out_weight, preferred_element_type=jnp.float32)
    summed = lax.psum_scatter(
        partial_sum.astype(jnp.bfloat16), "tensor", scatter_dimension=1, tiled=True
    ).astype(jnp.float32)
    result = jnp.where(is_valid[:, None], summed + packed.astype(jnp.float32), 0.0)
    return result.astype(jnp.bfloat16)


MESH = pl.DeviceIdType.MESH
CORES = 2
HALO = 16


def aligned(index, size):
    return pl.multiple_of(index * size, size)


def fused_kernel(
    cfg, pk_hbm, len_hbm, gain_hbm, tab_hbm, roll_hbm, w_in, k_in, o_in, out,
    pk_buf, len_buf, gain, tab, wbuf, kbuf, obuf, roll_in, sendb, recvb, packed, scaled, q_part, kv_part, q_recv, kv_recv, ctx,
    pos_buf, valid_buf, acc, sq_part, sq_recv, send_sems, recv_sems, local_sems,
):
    n_dp, n_t, length, feat, per_source = cfg
    chips = n_dp // CORES
    w_sub = feat // n_dp
    kd = k_in.shape[0]
    k_rows, k_cols = kd // chips, feat // CORES
    o_rows = o_in.shape[0]
    o_sub = o_rows // n_dp
    block = length // n_dp
    most = length // per_source
    rows = length // n_t
    qd = w_in.shape[1]
    me = lax.axis_index("dp")
    t = lax.axis_index("tensor")
    core = lax.rem(me, CORES)
    chip = lax.div(me, CORES)
    partner = chip * CORES + (CORES - 1 - core)

    def t_at(k):
        return lax.rem(t + k, n_t)

    def chip_at(k):
        return lax.rem(chip + k, chips) * CORES + core

    small = [
        pltpu.make_async_copy(source, target, local_sems.at[4 + i])
        for i, (source, target) in enumerate(
            (
                (pk_hbm, pk_buf),
                (len_hbm, len_buf),
                (gain_hbm.at[:, pl.ds(aligned(t, feat), feat)], gain),
                (tab_hbm, tab),
            )
        )
    ]
    load = pltpu.make_async_copy(roll_hbm, roll_in, local_sems.at[2])
    for copy in [*small, load]:
        copy.start()

    barrier = pltpu.get_barrier_semaphore()
    for k in range(1, n_dp):
        pl.semaphore_signal(
            barrier, inc=1, device_id=(lax.rem(me + k, n_dp), t), device_id_type=MESH
        )
    for k in range(1, n_t):
        pl.semaphore_signal(barrier, inc=1, device_id=(me, t_at(k)), device_id_type=MESH)
    pl.semaphore_wait(barrier, n_dp + n_t - 2)

    started = []

    def send(source, target, device):
        at = len(started)
        copy = pltpu.make_async_remote_copy(
            src_ref=source,
            dst_ref=target,
            send_sem=send_sems.at[at],
            recv_sem=recv_sems.at[at],
            device_id=device,
            device_id_type=MESH,
        )
        copy.start()
        started.append(copy)
        return copy

    def w_at(u, h, c):
        return wbuf.at[u, pl.ds(aligned(h * CORES + c, w_sub), w_sub)]

    def k_at(u, h, c):
        return kbuf.at[
            pl.ds(aligned(u * chips + h, k_rows), k_rows), pl.ds(aligned(c, k_cols), k_cols)
        ]

    def o_at(u, h, c):
        return obuf.at[u, pl.ds(aligned(h * CORES + c, o_sub), o_sub)]

    w_first, k_first, o_first = {}, {}, {}
    for k in range(1, n_t):
        to = t_at(k)
        k_first[k] = send(
            k_in.at[
                pl.ds(aligned(chip, k_rows), k_rows),
                pl.ds(aligned(to * CORES + core, k_cols), k_cols),
            ],
            k_at(t, chip, core),
            (me, to),
        )
    for k in range(1, n_t):
        to = t_at(k)
        w_first[k] = send(
            w_in.at[pl.ds(aligned(to * n_dp + me, w_sub), w_sub)], w_at(t, chip, core), (me, to)
        )
    own_w = pltpu.make_async_copy(
        w_in.at[pl.ds(aligned(t, feat), feat)], wbuf.at[t], local_sems.at[0]
    )
    own_w.start()
    own_k = pltpu.make_async_copy(
        k_in.at[:, pl.ds(aligned(t, feat), feat)],
        kbuf.at[pl.ds(aligned(t, kd), kd)],
        local_sems.at[3],
    )
    own_k.start()
    for k in range(1, n_t):
        to = t_at(k)
        o_first[k] = send(
            o_in.at[pl.ds(aligned(me, o_sub), o_sub), pl.ds(aligned(to, feat), feat)],
            o_at(t, chip, core),
            (me, to),
        )
    own_o = pltpu.make_async_copy(
        o_in.at[:, pl.ds(aligned(t, feat), feat)], obuf.at[t], local_sems.at[1]
    )
    own_o.start()

    down = lax.broadcasted_iota(jnp.int32, (length, length), 0).astype(jnp.float32)
    across = lax.broadcasted_iota(jnp.int32, (length, length), 1).astype(jnp.float32)

    def part(value, size):
        return jnp.floor((value + 0.5) * (1.0 / size))

    def pick(mask, value, axis):
        return jnp.sum(jnp.where(mask, value, 0.0), axis=axis, keepdims=True)

    same = part(down, per_source) == part(across, per_source)
    diagonal = down == across
    for copy in small:
        copy.wait()
    len_all = len_buf[...].astype(jnp.float32)
    source_of = part(down[:, :1], per_source)
    table = jnp.zeros((length, per_source), jnp.float32)
    for i in range(n_dp):
        table = jnp.where(source_of == float(i), len_all[i : i + 1, :], table)
    within = down[:, :per_source] - source_of * per_source
    len_c = pick(across[:, :per_source] == within, table, 1)
    len_r = pick(diagonal, len_c, 0)
    pk_r = pk_buf[...].astype(jnp.float32)
    pk_c = pick(diagonal, pk_r, 1)
    src_start = pick(same & (across < down), len_r, 1)
    chosen = down == pk_r
    q_len_r = pick(chosen, len_c, 0)
    q_start_r = pick(chosen, src_start, 0)
    q_len_c = pick(across == pk_c, len_r, 1)
    earlier = same & (down < across)
    doc_start_r = pick(earlier, q_len_c, 0)
    q_src_r = part(pk_r, per_source)
    slot_r = pick(earlier & (part(pk_c, per_source) == q_src_r), 1.0, 0)
    mine = me.astype(jnp.float32)
    across_1 = across[:1]
    down_1 = down[:, :1]
    owner_r = part(across_1, per_source)
    target = jnp.where(q_src_r == mine, owner_r * (per_source // n_dp) + slot_r, -1.0)
    group = part(down_1, most)
    match = target == group
    token = down_1 - group * most
    row_sent = jnp.where(token < pick(match, q_len_r, 1), pick(match, q_start_r, 1) + token, -1.0)
    take_send = (across == row_sent).astype(jnp.float32).astype(jnp.bfloat16)
    inside = (owner_r == mine) & (doc_start_r <= down) & (down < doc_start_r + q_len_r)
    is_valid = pick(inside, 1.0, 1)
    position = (down_1 - pick(inside, doc_start_r, 1)) * is_valid
    row_got = jnp.where(
        is_valid > 0.0, pick(inside, q_src_r * block + slot_r * most, 1) + position, -1.0
    )
    take_recv = (across == row_got).astype(jnp.float32).astype(jnp.bfloat16)
    pos_buf[:HALO, :] = jnp.zeros((HALO, HD), jnp.float32)
    pos_buf[HALO:, :] = jnp.broadcast_to(position, (length, HD))
    valid_buf[...] = jnp.broadcast_to(is_valid, (length, HD))

    tile = 256
    tiles = feat // tile

    def send_tile(i, carry):
        at = pl.ds(aligned(i, tile), tile)
        sendb[:, at] = jnp.dot(
            take_send, roll_in[:, at], preferred_element_type=jnp.float32
        ).astype(jnp.bfloat16)
        return carry

    load.wait()
    lax.fori_loop(0, tiles, send_tile, 0)

    rows_of = {}
    for k in range(1, n_dp):
        to = lax.rem(me + k, n_dp)
        rows_of[k] = send(
            sendb.at[pl.ds(aligned(to, block), block)],
            recvb.at[pl.ds(aligned(me, block), block)],
            (to, t),
        )
    keep = pl.ds(aligned(me, block), block)
    recvb[keep, :] = sendb[keep, :]

    def spread(at, first, j):
        first[j].wait_recv()
        ref = at(t_at(n_t - j), chip, core)
        return [send(ref, ref, (chip_at(k), t)) for k in range(1, chips)]

    def share(at, hops, j):
        last = []
        for k in range(chips):
            if k:
                hops[k - 1].wait_recv()
            ref = at(t_at(n_t - j), lax.rem(chip + chips - k, chips), core)
            last.append(send(ref, ref, (partner, t)))
        return last

    others = range(1, n_t)
    k_hops = {j: spread(k_at, k_first, j) for j in others}
    w_hops = {1: spread(w_at, w_first, 1)}

    for k in range(1, n_dp):
        rows_of[k].wait_recv()

    def pack_tile(i, total):
        at = pl.ds(aligned(i, tile), tile)
        x = jnp.dot(take_recv, recvb[:, at], preferred_element_type=jnp.float32)
        packed[:, at] = x.astype(jnp.bfloat16)
        g = gain[:, at]
        scaled[:, at] = (x * g).astype(jnp.bfloat16)
        return total + jnp.sum(x * x, axis=1, keepdims=True)

    squares = lax.fori_loop(0, tiles, pack_tile, jnp.zeros((length, 1), jnp.float32))
    kv_part[:HALO, :] = jnp.zeros((HALO, 2 * HD), jnp.bfloat16)
    sq_part[...] = jnp.broadcast_to(pick(diagonal, squares, 0), (8, length))
    shares = []

    def reduce_rows(part_ref, recv_ref, extra, cols):
        for k in others:
            to = t_at(k)
            shares.append(
                send(
                    part_ref.at[pl.ds(aligned(to, rows), rows + extra), cols],
                    recv_ref.at[k - 1, :, cols],
                    (me, to),
                )
            )

    def project(j):
        u = t_at(n_t - j)
        cols = pl.ds(aligned(u, qd), qd)
        q_part[:, cols] = jnp.dot(
            scaled[...], wbuf[u], preferred_element_type=jnp.float32
        ).astype(jnp.bfloat16)
        reduce_rows(q_part, q_recv, 0, cols)

    own_w.wait()
    own_k.wait()
    for k in others:
        shares.append(send(sq_part, sq_recv.at[k - 1], (me, t_at(k))))
    project(n_t)
    for j in others[1:]:
        w_hops[j] = spread(w_at, w_first, j)
    k_last = [copy for j in others for copy in share(k_at, k_hops[j], j)]
    for copy in k_last:
        copy.wait_recv()
    kv_part[HALO:, : 2 * HD] = lax.dot_general(
        scaled[...], kbuf[...], (((1,), (1,)), ((), ())), preferred_element_type=jnp.float32
    ).astype(jnp.bfloat16)
    reduce_rows(kv_part, kv_recv, HALO, pl.ds(0, 2 * HD))
    w_last = share(w_at, w_hops[1], 1)
    o_hops = {}
    for j in others:
        if j + 1 in w_hops:
            following = share(w_at, w_hops[j + 1], j + 1)
        for copy in w_last:
            copy.wait_recv()
        w_last = following
        project(j)
        o_hops[j] = spread(o_at, o_first, j)
    for copy in shares:
        copy.wait_recv()

    keys_at = pl.ds(aligned(t, rows), rows + HALO)
    queries_at = pl.ds(aligned(t, rows), rows)
    kv = kv_part[keys_at, :].astype(jnp.float32)
    for k in range(n_t - 1):
        kv += kv_recv[k].astype(jnp.float32)
    sq = sq_part[:1, :]
    for k in range(n_t - 1):
        sq += sq_recv[k, :1, :]
    row_at = lax.broadcasted_iota(jnp.int32, (rows + HALO, length), 0) + (t * rows - HALO)
    sums = pick(lax.broadcasted_iota(jnp.int32, (rows + HALO, length), 1) == row_at, sq, 1)
    inverse = lax.rsqrt(sums / (feat * n_t) + epsilon)
    kv_bf = (kv[:, : 2 * HD] * inverse).astype(jnp.bfloat16)
    values = kv_bf[:, HD:]
    pos = pos_buf[keys_at, :]
    cosine = jnp.zeros((rows + HALO, HD), jnp.float32)
    sine = jnp.zeros((rows + HALO, HD), jnp.float32)
    for m in range(most):
        at_m = pos == float(m)
        cosine = jnp.where(at_m, tab[m : m + 1, :], cosine)
        sine = jnp.where(at_m, tab[most + m : most + m + 1, :], sine)

    def turn(v, c, s):
        return v * c + pltpu.roll(v, HD // 2, 1) * s

    k_rot = turn(kv_bf[:, :HD].astype(jnp.float32), cosine, sine).astype(jnp.bfloat16)
    q_down = lax.broadcasted_iota(jnp.int32, (rows, rows + HALO), 0).astype(jnp.float32)
    k_across = lax.broadcasted_iota(jnp.int32, (rows, rows + HALO), 1).astype(jnp.float32) - HALO
    allowed = (k_across <= q_down) & (k_across >= q_down - pos[HALO:, :1])
    gathers = []
    heads = q_part.shape[1] // HD
    for h in range(heads):
        cols = slice(h * HD, (h + 1) * HD)
        q = q_part[queries_at, cols].astype(jnp.float32)
        for k in range(n_t - 1):
            q += q_recv[k, :, cols].astype(jnp.float32)
        q_rot = turn(q * inverse[HALO:], cosine[HALO:], sine[HALO:]).astype(jnp.bfloat16)
        scores = lax.dot_general(
            q_rot, k_rot, (((1,), (1,)), ((), ())), preferred_element_type=jnp.float32
        ) * (1.0 / math.sqrt(HD))
        scores = jnp.where(allowed, scores, -jnp.inf)
        exponent = jnp.exp(scores - jnp.max(scores, axis=1, keepdims=True))
        weights = (exponent / jnp.sum(exponent, axis=1, keepdims=True)).astype(jnp.bfloat16)
        ctx[queries_at, cols] = jnp.dot(
            weights, values, preferred_element_type=jnp.float32
        ).astype(jnp.bfloat16)
        if (h + 1) % (heads // n_t) == 0:
            at = ctx.at[queries_at, pl.ds((h + 1 - heads // n_t) * HD, heads // n_t * HD)]
            for k in others:
                gathers.append(send(at, at, (me, t_at(k))))

    o_last = [copy for j in others for copy in share(o_at, o_hops[j], j)]
    own_o.wait()
    for copy in o_last:
        copy.wait_recv()

    for u in range(n_t):
        for copy in gathers[u * (n_t - 1) : (u + 1) * (n_t - 1)]:
            copy.wait_recv()

        def out_tile(i, carry, u=u):
            at = pl.ds(aligned(i, tile), tile)
            total = packed[:, at].astype(jnp.float32) if u == 0 else acc[:, at]
            total += jnp.dot(
                ctx[:, u * o_rows : (u + 1) * o_rows],
                obuf[u, :, at],
                preferred_element_type=jnp.float32,
            )
            if u < n_t - 1:
                acc[:, at] = total
            else:
                out[:, at] = jnp.where(valid_buf[:, :1] > 0.0, total, 0.0).astype(jnp.bfloat16)
            return carry

        lax.fori_loop(0, tiles, out_tile, 0)
    for copy in started:
        copy.wait_send()


def fused_body(rollout, lengths, packing, norm_gain, query_weight, keyval_weight, out_weight):
    n_dp, n_t = lax.axis_size("dp"), lax.axis_size("tensor")
    length, feat = rollout.shape
    per_source = lengths.shape[1]
    most = length // per_source
    qd, kd = query_weight.shape[1], keyval_weight.shape[1]
    frequency = np.float32(rope_base) ** (-np.arange(HD // 2, dtype=np.float32) * 2.0 / HD)
    angles = np.arange(most, dtype=np.float32)[:, None] * frequency[None, :].astype(np.float32)
    cos_tab = np.concatenate([np.cos(angles)] * 2, axis=1).astype(np.float32)
    sin_tab = np.concatenate([-np.sin(angles), np.sin(angles)], axis=1).astype(np.float32)
    rows = length // n_t
    chips = n_dp // CORES
    copies = 3 * (n_t - 1) * (1 + chips - 1 + chips) + (n_dp - 1) + (2 + 2 * n_t) * (n_t - 1)
    vmem = pl.BlockSpec(memory_space=pltpu.VMEM)
    hbm = pl.BlockSpec(memory_space=pl.ANY)
    bf, f32 = jnp.bfloat16, jnp.float32
    return pl.pallas_call(
        functools.partial(fused_kernel, (n_dp, n_t, length, feat, per_source)),
        out_shape=jax.ShapeDtypeStruct((length, feat), bf),
        in_specs=[hbm] * 8,
        out_specs=vmem,
        scratch_shapes=[
            pltpu.VMEM((1, packing.shape[0]), jnp.int32),
            pltpu.VMEM(lengths.shape, jnp.int32),
            pltpu.VMEM((1, feat), f32),
            pltpu.VMEM((2 * most, HD), f32),
            pltpu.VMEM((n_t, feat, qd), bf),
            pltpu.VMEM((n_t * kd, feat), bf),
            pltpu.VMEM((n_t, out_weight.shape[0], feat), bf),
            pltpu.VMEM((length, feat), bf),
            pltpu.VMEM((length, feat), bf),
            pltpu.VMEM((length, feat), bf),
            pltpu.VMEM((length, feat), bf),
            pltpu.VMEM((length, feat), bf),
            pltpu.VMEM((length, n_t * qd), bf),
            pltpu.VMEM((length + HALO, 2 * HD), bf),
            pltpu.VMEM((n_t - 1, rows, n_t * qd), bf),
            pltpu.VMEM((n_t - 1, rows + HALO, 2 * HD), bf),
            pltpu.VMEM((length, n_t * qd), bf),
            pltpu.VMEM((length + HALO, HD), f32),
            pltpu.VMEM((length, HD), f32),
            pltpu.VMEM((length, feat), f32),
            pltpu.VMEM((8, length), f32),
            pltpu.VMEM((n_t - 1, 8, length), f32),
            pltpu.SemaphoreType.DMA((copies,)),
            pltpu.SemaphoreType.DMA((copies,)),
            pltpu.SemaphoreType.DMA((8,)),
        ],
        compiler_params=pltpu.CompilerParams(
            collective_id=0, has_side_effects=True, vmem_limit_bytes=60 * 1024 * 1024
        ),
    )(
        packing[None, :], lengths, norm_gain[None, :],
        jnp.asarray(np.concatenate([cos_tab, sin_tab])), rollout, query_weight,
        keyval_weight.T, out_weight,
    )


def body(rollout, lengths, packing, norm_gain, query_weight, keyval_weight, out_weight):
    n_dp, n_t = lax.axis_size("dp"), lax.axis_size("tensor")
    length, feat = rollout.shape
    qd, kd = query_weight.shape[1], keyval_weight.shape[1]
    fits = (
        kd * n_t == 2 * HD
        and n_t == 4
        and kd % (HALO * n_dp // CORES) == 0
        and feat % (128 * CORES) == 0
        and n_dp % CORES == 0
        and length % (n_t * HALO) == 0
        and packing.shape[0] == length
        and (length // n_dp) % HALO == 0
        and feat % 512 == 0
        and lengths.shape[1] % n_dp == 0
    )
    chosen = fused_body if fits else plain_body
    return chosen(rollout, lengths, packing, norm_gain, query_weight, keyval_weight, out_weight)


def solution(mesh):
    in_specs = (
        P("dp", "tensor"),
        P(),
        P(),
        P(),
        P(None, "tensor"),
        P(None, "tensor"),
        P("tensor", None),
    )
    out_specs = P("dp", "tensor")
    return jax.shard_map(body, mesh=mesh, in_specs=in_specs, out_specs=out_specs, check_vma=False)
```
